32 devices in a mesh: gx: 4 (over z), gy: 8 (over y, x, core).
Axes of the slice: x: 2, y: 2, z: 4, core: 2. Of those that a mesh axis runs over, the one named last changes fastest.
Arguments:
- radiance: bfloat16 [2048, 16, 128], P(('gx', 'gy')), may hold values from 0.049804688 to 2
- emission: float32 [2048, 16, 128], P(('gx', 'gy')), may hold values from 0.01 to 1
- reflectance: float32 [2048, 16, 128], P(('gx', 'gy')), may hold values from 0.1 to 0.9
- patch_area: float32 [2048, 128], P(('gx', 'gy')), may hold values from 0.25 to 4
- form_factor: bfloat16 [4096, 128, 128], P(('gx', 'gy')), may hold values from 0.00049972534 to 0.014953613
- source_index: int32 [32, 128], P(('gx', 'gy')), may hold values from 0 to 63
- target_index: int32 [32, 128], P(('gx', 'gy')), may hold values from 0 to 63
- block_index: int32 [32, 128], P(('gx', 'gy')), may hold values from 0 to 127, each once within a row
- valid_count: int32 [32, 32], P(('gx', 'gy')), may hold values from 0 to 4, as said below
Outputs:
- new_radiance: float32 [2048, 16, 128], P(('gx', 'gy'))
The draws below stay inside these ranges and needn't reach their ends.
Inputs may be any that keep to these rules, and one draw needn't show every extreme that they name: `valid_count`: entry [d, p] is the number of live slots among the 4 slots of device d toward peer p, the live ones first; every row has an entry equal to 4. `block_index`: each row is a permutation of 0 to 127.
All inputs are finite; a program needn't handle non-finite values.
Results may differ from the reference program's by a relative error of at most 0.0012.
Values may be sent and summed in bfloat16 or wider, within the bound.
A program may use at most 128 MiB of HBM per device.

```python
import math
import jax
import jax.numpy as jnp
from jax import lax

PATCH = 128
BANDS = 16
CL_DEV = 64
SLOTS = 4
CLUSTERS = 2048
LINKS = 128
DEVICES = 32


def draw_valid_count(key, part):
    base_key = jax.random.fold_in(key, 7)
    heavy_key, count_key, full_key = jax.random.split(base_key, 3)
    heavy_flag = jax.random.randint(heavy_key, (DEVICES, 1), 0, 4) == 0
    lowest = jnp.where(heavy_flag, SLOTS // 2, 0)
    highest = jnp.where(heavy_flag, SLOTS, SLOTS // 2)
    raw_bits = jax.random.randint(count_key, (DEVICES, DEVICES), 0, 1 << 20)
    counts = lowest + raw_bits % (highest - lowest + 1)
    full_peer = jax.random.randint(full_key, (DEVICES,), 0, DEVICES)
    columns = jnp.arange(DEVICES, dtype=jnp.int32)
    counts = jnp.where(columns[None, :] == full_peer[:, None], SLOTS, counts)
    return counts.astype(jnp.int32)


def place_ends(array, rng, smallest, top_value):
    spot = [jax.random.randint(jax.random.fold_in(rng, axis), (), 0, length) for axis, length in enumerate(array.shape)]
    main_axis = array.shape.index(max(array.shape))
    next_to = spot[:main_axis] + [(spot[main_axis] + 1) % array.shape[main_axis]] + spot[main_axis + 1:]
    return array.at[tuple(spot)].set(smallest).at[tuple(next_to)].set(top_value)


def levels(own_key, shape, cuts, low, top_value):
    loudness = 1.0
    for axis_at, shards_of in cuts:
        steps = jax.random.uniform(jax.random.fold_in(jax.random.fold_in(own_key, 6), axis_at), (shards_of,), jnp.float32, low / len(cuts), top_value / len(cuts))
        loudness = loudness * jnp.repeat(jnp.exp(steps), shape[axis_at] // shards_of).reshape((-1,) + (1,) * (len(shape) - 1 - axis_at))
    return loudness


def setup_inputs(seed: int = 0) -> dict:
    seeds = jax.random.split(jax.random.key(seed), 10)
    return {
        "radiance": jnp.clip(jnp.exp(math.log(2.0) - 3.6927934 * jax.random.uniform(seeds[0], (CLUSTERS, BANDS, PATCH), jnp.float32) ** levels(seeds[0], (CLUSTERS, BANDS, PATCH), ((0, 32),), -0.2, 0.2)), 0.049804688, 2.0).astype(jnp.bfloat16),
        "emission": jnp.clip(jnp.exp(math.log(1.0) - 4.6051702 * jax.random.uniform(seeds[1], (CLUSTERS, BANDS, PATCH), jnp.float32) ** levels(seeds[1], (CLUSTERS, BANDS, PATCH), ((0, 32),), -0.2, 0.2)), 0.01, 1.0),
        "reflectance": jnp.clip(jnp.exp(math.log(0.9) - 2.1972245 * jax.random.uniform(seeds[2], (CLUSTERS, BANDS, PATCH), jnp.float32) ** levels(seeds[2], (CLUSTERS, BANDS, PATCH), ((0, 32),), -0.2, 0.2)), 0.1, 0.9),
        "patch_area": jnp.clip(jnp.exp(math.log(4.0) - 2.7725887 * jax.random.uniform(seeds[3], (CLUSTERS, PATCH), jnp.float32) ** levels(seeds[3], (CLUSTERS, PATCH), ((0, 32),), -0.2, 0.2)), 0.25, 4.0),
        "form_factor": jnp.clip(jnp.exp(math.log(0.014953613) - 3.3986496 * jax.random.uniform(seeds[4], (DEVICES * LINKS, PATCH, PATCH), jnp.float32) ** levels(seeds[4], (DEVICES * LINKS, PATCH, PATCH), ((0, 32),), -0.2, 0.2)), 0.00049972534, 0.014953613).astype(jnp.bfloat16),
        "source_index": place_ends(jax.random.randint(seeds[5], (DEVICES, LINKS), 0, CL_DEV), jax.random.fold_in(seeds[5], 1), 0, CL_DEV - 1).astype(jnp.int32),
        "target_index": place_ends(jax.random.randint(seeds[6], (DEVICES, LINKS), 0, CL_DEV), jax.random.fold_in(seeds[6], 1), 0, CL_DEV - 1).astype(jnp.int32),
        "block_index": jax.vmap(lambda own: jax.random.permutation(own, LINKS))(jax.random.split(seeds[7], DEVICES)).reshape((DEVICES, LINKS)).astype(jnp.int32),
        "valid_count": draw_valid_count(jax.random.fold_in(seeds[9], 71), 0),
    }


def reference(radiance, emission, reflectance, patch_area, form_factor, source_index, target_index, block_index, valid_count):
    rad_full = radiance.astype(jnp.float32)
    weighted = (patch_area[:, None, :] * rad_full).astype(jnp.bfloat16)
    weighted_full = weighted.astype(jnp.float32)
    blocks = form_factor.reshape(DEVICES, LINKS, PATCH, PATCH)
    device_ids = jnp.arange(DEVICES, dtype=jnp.int32)

    def step_device(carry, inputs):
        gathered, returned = carry
        device, block_row, source_row, target_row, stored_blocks, live_count = inputs
        position = jnp.arange(LINKS, dtype=jnp.int32)
        peer_ids = (position // SLOTS).astype(jnp.int32)
        live_mask = ((position % SLOTS) < live_count[peer_ids]).astype(jnp.float32)
        source_cluster = (peer_ids * CL_DEV + source_row).astype(jnp.int32)
        target_cluster = (device * CL_DEV + target_row).astype(jnp.int32)
        chosen = stored_blocks[block_row].astype(jnp.float32)
        forward = jnp.einsum("lij,lbj->lbi", chosen, rad_full[source_cluster]) * live_mask[:, None, None]
        backward = jnp.einsum("lij,lbi->lbj", chosen, weighted_full[target_cluster]).astype(jnp.bfloat16)
        backward = lax.optimization_barrier(backward)
        backward = backward.astype(jnp.float32) * live_mask[:, None, None]
        gathered = gathered.at[target_cluster].add(forward)
        returned = returned.at[source_cluster].add(backward)
        return (gathered, returned), None

    zeros_sum = jnp.zeros((CLUSTERS, BANDS, PATCH), jnp.float32)
    (gathered, returned), _ = lax.scan(step_device, (zeros_sum, zeros_sum),
                                       (device_ids, block_index, source_index, target_index, blocks, valid_count))
    irradiance = gathered + returned / patch_area[:, None, :]
    return emission + reflectance * irradiance
```

```python
import functools

import jax
import jax.numpy as jnp
from jax import lax
from jax.experimental import pallas as pl
from jax.experimental.pallas import tpu as pltpu
from jax.sharding import PartitionSpec as P

MESH = pl.DeviceIdType.MESH
GROUP = 4
LANES = 128
F32 = jnp.float32
BF16 = jnp.bfloat16


def exchange(
    n,
    inner,
    block_ref,
    target_ref,
    count_ref,
    source_ref,
    rad_ref,
    area_ref,
    form_hbm,
    fwd_ref,
    arrived_ref,
    asked_out,
    form_ref,
    weighted_ref,
    bwd_ref,
    served_ref,
    fetched_ref,
    asked_vmem,
    asked_ref,
    form_sem,
    asked_sem,
    send_sems,
    idx_sem,
    bwd_sem,
    rad_sem,
):
    me = lax.axis_index("gx") * inner + lax.axis_index("gy")
    links = block_ref.shape[1]
    slots = links // n
    clusters = rad_ref.shape[0]
    parts = form_sem.shape[0]
    step = links // parts

    def coords(p):
        return (p // inner, p % inner)

    def form_copy(i):
        rows = pl.ds(i * step, step)
        return pltpu.make_async_copy(form_hbm.at[rows], form_ref.at[rows], form_sem.at[i])

    for i in range(parts):
        form_copy(i).start()

    barrier = pltpu.get_barrier_semaphore()

    def greet(k, c):
        pl.semaphore_signal(
            barrier, inc=1, device_id=coords((me + k) % n), device_id_type=MESH
        )
        return c

    lax.fori_loop(1, n, greet, 0)

    def weigh(c, carry):
        area = area_ref[pl.ds(c, 1), :]
        weighted_ref[c] = (area * rad_ref[c].astype(F32)).astype(BF16)
        return carry

    lax.fori_loop(0, clusters, weigh, 0, unroll=8)

    pl.semaphore_wait(barrier, n - 1)

    width = asked_vmem.shape[2]

    def lane_base(p):
        if links == width:
            return 0
        return pl.multiple_of(p * slots // width * width, width)

    def idx_copy(k):
        p = (me + k) % n
        return pltpu.make_async_remote_copy(
            src_ref=source_ref.at[:, pl.ds(lane_base(p), width)],
            dst_ref=asked_vmem.at[me],
            send_sem=send_sems.at[0],
            recv_sem=idx_sem.at[k],
            device_id=coords(p),
            device_id_type=MESH,
        )

    def send_idx(k, c):
        idx_copy(k).start()
        return c

    lax.fori_loop(1, n, send_idx, 0)
    asked_vmem[me] = source_ref[:, pl.ds(lane_base(me), width)]

    def bwd_copy(k):
        p = (me + k) % n
        return pltpu.make_async_remote_copy(
            src_ref=bwd_ref.at[pl.ds(p * slots, slots)],
            dst_ref=arrived_ref.at[pl.ds(me * slots, slots)],
            send_sem=send_sems.at[1],
            recv_sem=bwd_sem.at[k],
            device_id=coords(p),
            device_id_type=MESH,
        )

    def rad_copy(k):
        p = (me + k) % n
        return pltpu.make_async_remote_copy(
            src_ref=served_ref.at[pl.ds(p * slots, slots)],
            dst_ref=fetched_ref.at[pl.ds(me * slots, slots)],
            send_sem=send_sems.at[2],
            recv_sem=rad_sem.at[k],
            device_id=coords(p),
            device_id_type=MESH,
        )

    def live_of(p, s):
        return jnp.where(s < count_ref[0, p], 1.0, 0.0).astype(F32)

    for i in range(parts):
        form_copy(i).wait()

    def backward(t, c):
        for u in range(GROUP):
            p = (me + t * GROUP + u) % n
            for s in range(slots):
                l = p * slots + s
                form = form_ref[block_ref[0, l]]
                seen = weighted_ref[target_ref[0, l]]
                got = jnp.dot(seen, form, preferred_element_type=F32)
                bwd_ref[l] = (got * live_of(p, s)).astype(BF16)
        for u in range(GROUP):
            k = t * GROUP + u

            @pl.when(k != 0)
            def _():
                bwd_copy(k).start()

        return c

    lax.fori_loop(0, n // GROUP, backward, 0)

    def wait_idx(k, c):
        idx_copy(k).wait_recv()
        return c

    lax.fori_loop(1, n, wait_idx, 0)
    to_smem = pltpu.make_async_copy(asked_vmem, asked_ref, asked_sem)
    to_smem.start()
    to_smem.wait()
    base = me * slots % width

    def serve(k, c):
        p = (me + k) % n
        for s in range(slots):
            served_ref[p * slots + s] = rad_ref[asked_ref[p, 0, base + s]]
            asked_out[0, p * slots + s] = asked_ref[p, 0, base + s]

        @pl.when(k != 0)
        def _():
            rad_copy(k).start()

        return c

    lax.fori_loop(0, n, serve, 0)
    own = pl.ds(me * slots, slots)
    fetched_ref[own] = served_ref[own]
    arrived_ref[own] = bwd_ref[own]

    def forward(t, c):
        for u in range(GROUP):
            k = t * GROUP + u

            @pl.when(k != 0)
            def _():
                rad_copy(k).wait_recv()

        for u in range(GROUP):
            p = (me + n - t * GROUP - u) % n
            for s in range(slots):
                l = p * slots + s
                form = form_ref[block_ref[0, l]]
                got = lax.dot_general(
                    fetched_ref[l], form, (((1,), (1,)), ((), ())), preferred_element_type=F32
                )
                fwd_ref[l] = got * live_of(p, s)
        return c

    lax.fori_loop(0, n // GROUP, forward, 0)

    def wait_bwd(k, c):
        bwd_copy(k).wait_recv()
        return c

    lax.fori_loop(1, n, wait_bwd, 0)
    most = pl.ds(0, (n - 1) * slots)
    for buf, which in ((bwd_ref, 1), (served_ref, 2)):
        pltpu.make_async_copy(buf.at[most], buf.at[most], send_sems.at[which]).wait()
    rows = asked_vmem.at[pl.ds(0, n - 1)]
    pltpu.make_async_copy(rows, rows, send_sems.at[0]).wait()


def combine(
    target_ref, asked_ref, fwd_ref, arrived_ref, em_ref, refl_ref, area_ref, out_ref, gath, ret
):
    clusters = em_ref.shape[0]
    links = fwd_ref.shape[0]

    def clear(c, carry):
        gath[c] = jnp.zeros(gath.shape[1:], F32)
        ret[c] = jnp.zeros(ret.shape[1:], F32)
        return carry

    lax.fori_loop(0, clusters, clear, 0, unroll=8)

    def scatter(l, carry):
        t = target_ref[0, l]
        s = asked_ref[0, l]
        gath[t] += fwd_ref[l]
        ret[s] += arrived_ref[l].astype(F32)
        return carry

    lax.fori_loop(0, links, scatter, 0, unroll=8)

    def finish(c, carry):
        area = area_ref[pl.ds(c, 1), :]
        out_ref[c] = em_ref[c] + refl_ref[c] * (gath[c] + ret[c] / area)
        return carry

    lax.fori_loop(0, clusters, finish, 0, unroll=8)


def solution(mesh):
    outer, inner = mesh.shape["gx"], mesh.shape["gy"]
    n = outer * inner

    def shards(
        radiance,
        emission,
        reflectance,
        patch_area,
        form_factor,
        source_index,
        target_index,
        block_index,
        valid_count,
    ):
        clusters, bands, patches = radiance.shape
        links = source_index.shape[1]
        slots = links // n
        tile = (bands, patches)
        vm = pl.BlockSpec(memory_space=pltpu.VMEM)
        sm = pl.BlockSpec(memory_space=pltpu.SMEM)
        hbm = pl.BlockSpec(memory_space=pl.ANY)
        width = min(links, LANES)
        parts = 4
        fwd, arrived, asked = pl.pallas_call(
            functools.partial(exchange, n, inner),
            out_shape=(
                jax.ShapeDtypeStruct((links,) + tile, F32),
                jax.ShapeDtypeStruct((links,) + tile, BF16),
                jax.ShapeDtypeStruct((1, links), jnp.int32),
            ),
            in_specs=[sm, sm, sm, vm, vm, vm, hbm],
            out_specs=(vm, vm, sm),
            scratch_shapes=[
                pltpu.VMEM(form_factor.shape, BF16),
                pltpu.VMEM((clusters,) + tile, BF16),
                pltpu.VMEM((links,) + tile, BF16),
                pltpu.VMEM((links,) + tile, BF16),
                pltpu.VMEM((links,) + tile, BF16),
                pltpu.VMEM((n, 1, width), jnp.int32),
                pltpu.SMEM((n, 1, width), jnp.int32),
                pltpu.SemaphoreType.DMA((parts,)),
                pltpu.SemaphoreType.DMA,
                pltpu.SemaphoreType.DMA((3,)),
                pltpu.SemaphoreType.DMA((n,)),
                pltpu.SemaphoreType.DMA((n,)),
                pltpu.SemaphoreType.DMA((n,)),
            ],
            compiler_params=pltpu.CompilerParams(
                collective_id=0, has_side_effects=True, vmem_limit_bytes=60 * 1024 * 1024
            ),
            name="exchange",
        )(
            block_index,
            target_index,
            valid_count,
            source_index,
            radiance,
            patch_area,
            form_factor,
        )
        return pl.pallas_call(
            combine,
            out_shape=jax.ShapeDtypeStruct((clusters,) + tile, F32),
            in_specs=[sm, sm, vm, vm, vm, vm, vm],
            out_specs=vm,
            scratch_shapes=[pltpu.VMEM((clusters,) + tile, F32)] * 2,
            compiler_params=pltpu.CompilerParams(vmem_limit_bytes=24 * 1024 * 1024),
            name="combine",
        )(target_index, asked, fwd, arrived, emission, reflectance, patch_area)

    spec3 = P(("gx", "gy"), None, None)
    spec2 = P(("gx", "gy"), None)
    return jax.shard_map(
        shards,
        mesh=mesh,
        in_specs=(spec3, spec3, spec3, spec2, spec3, spec2, spec2, spec2, spec2),
        out_specs=spec3,
        check_vma=False,
    )
```

```python
import functools

import jax
import jax.numpy as jnp
from jax import lax
from jax.experimental import pallas as pl
from jax.experimental.pallas import tpu as pltpu
from jax.sharding import PartitionSpec as P

MESH = pl.DeviceIdType.MESH
GROUP = 4
LANES = 128
EXCHANGE_MIB = 60
COMBINE_MIB = 60
F32 = jnp.float32
BF16 = jnp.bfloat16


def exchange(
    n,
    inner,
    block_hbm,
    target_hbm,
    count_hbm,
    source_hbm,
    rad_hbm,
    area_hbm,
    form_hbm,
    fwd_hbm,
    arrived_hbm,
    asked_hbm,
    block_ref,
    target_ref,
    count_ref,
    source_ref,
    rad_ref,
    area_ref,
    form_ref,
    weighted_ref,
    bwd_ref,
    served_ref,
    fetched_ref,
    fwd_ref,
    asked_vmem,
    asked_ref,
    form_sem,
    in_sem,
    out_sem,
    send_sems,
    idx_sem,
    bwd_sem,
    rad_sem,
):
    me = lax.axis_index("gx") * inner + lax.axis_index("gy")
    links = block_ref.shape[1]
    slots = links // n
    clusters = rad_ref.shape[0]
    parts = form_sem.shape[0]
    step = links // parts

    def coords(p):
        return (p // inner, p % inner)

    loads = [
        pltpu.make_async_copy(src, dst, in_sem.at[i])
        for i, (src, dst) in enumerate(
            (
                (rad_hbm, rad_ref),
                (area_hbm, area_ref),
                (block_hbm, block_ref),
                (target_hbm, target_ref),
                (count_hbm, count_ref),
                (source_hbm, source_ref),
            )
        )
    ]
    forms = [
        pltpu.make_async_copy(
            form_hbm.at[pl.ds(i * step, step)], form_ref.at[pl.ds(i * step, step)], form_sem.at[i]
        )
        for i in range(parts)
    ]
    for load in loads + forms:
        load.start()

    barrier = pltpu.get_barrier_semaphore()

    def greet(k, c):
        pl.semaphore_signal(
            barrier, inc=1, device_id=coords((me + k) % n), device_id_type=MESH
        )
        return c

    lax.fori_loop(1, n, greet, 0)

    for load in loads:
        load.wait()

    def weigh(c, carry):
        area = area_ref[pl.ds(c, 1), :]
        weighted_ref[c] = (area * rad_ref[c].astype(F32)).astype(BF16)
        return carry

    lax.fori_loop(0, clusters, weigh, 0, unroll=8)

    width = asked_vmem.shape[2]

    def lane_base(p):
        if links == width:
            return 0
        return pl.multiple_of(p * slots // width * width, width)

    def idx_copy(k):
        p = (me + k) % n
        return pltpu.make_async_remote_copy(
            src_ref=source_ref.at[:, pl.ds(lane_base(p), width)],
            dst_ref=asked_vmem.at[me],
            send_sem=send_sems.at[0],
            recv_sem=idx_sem.at[k],
            device_id=coords(p),
            device_id_type=MESH,
        )

    def bwd_copy(k):
        p = (me + k) % n
        return pltpu.make_async_remote_copy(
            src_ref=bwd_ref.at[pl.ds(p * slots, slots)],
            dst_ref=arrived_hbm.at[pl.ds(me * slots, slots)],
            send_sem=send_sems.at[1],
            recv_sem=bwd_sem.at[k],
            device_id=coords(p),
            device_id_type=MESH,
        )

    def rad_copy(k):
        p = (me + k) % n
        return pltpu.make_async_remote_copy(
            src_ref=served_ref.at[pl.ds(p * slots, slots)],
            dst_ref=fetched_ref.at[pl.ds(me * slots, slots)],
            send_sem=send_sems.at[2],
            recv_sem=rad_sem.at[k],
            device_id=coords(p),
            device_id_type=MESH,
        )

    def live_of(p, s):
        return jnp.where(s < count_ref[0, p], 1.0, 0.0).astype(F32)

    for form in forms:
        form.wait()

    def back(t):
        for u in range(GROUP):
            p = (me + 1 + t * GROUP + u) % n
            for s in range(slots):
                l = p * slots + s
                form = form_ref[block_ref[0, l]]
                seen = weighted_ref[target_ref[0, l]]
                got = jnp.dot(seen, form, preferred_element_type=F32)
                bwd_ref[l] = (got * live_of(p, s)).astype(BF16)

    def back_only(t, c):
        back(t)
        return c

    def send_bwd(k, c):
        bwd_copy(k).start()
        return c

    def back_send(t, c):
        back(t)
        for u in range(GROUP):
            k = 1 + t * GROUP + u

            @pl.when(k != n)
            def _():
                bwd_copy(k).start()

        return c

    early = n // GROUP // 2
    lax.fori_loop(0, early, back_only, 0)
    pl.semaphore_wait(barrier, n - 1)

    def send_idx(k, c):
        idx_copy(k).start()
        return c

    lax.fori_loop(1, n, send_idx, 0)
    lax.fori_loop(1, 1 + early * GROUP, send_bwd, 0)
    asked_vmem[me] = source_ref[:, pl.ds(lane_base(me), width)]
    lax.fori_loop(early, n // GROUP, back_send, 0)

    own = pl.ds(me * slots, slots)
    keep_own = pltpu.make_async_copy(bwd_ref.at[own], arrived_hbm.at[own], out_sem.at[0])
    keep_own.start()

    def wait_idx(k, c):
        idx_copy(k).wait_recv()
        return c

    lax.fori_loop(1, n, wait_idx, 0)
    to_smem = pltpu.make_async_copy(asked_vmem, asked_ref, out_sem.at[1])
    to_smem.start()
    to_smem.wait()
    base = me * slots % width

    def serve(k, c):
        p = (me + k) % n
        for s in range(slots):
            served_ref[p * slots + s] = rad_ref[asked_ref[p, 0, base + s]]

        @pl.when(k != n)
        def _():
            rad_copy(k).start()

        return c

    lax.fori_loop(1, n + 1, serve, 0)
    for s in range(slots):
        fetched_ref[me * slots + s] = served_ref[me * slots + s]
    keep_asked = pltpu.make_async_copy(asked_vmem, asked_hbm, out_sem.at[1])
    keep_asked.start()

    def fwd_copy(k):
        mine = pl.ds((me + n - k) % n * slots, slots)
        return pltpu.make_async_copy(fwd_ref.at[mine], fwd_hbm.at[mine], out_sem.at[2])

    def forward(t, c):
        for u in range(GROUP):
            k = t * GROUP + u

            @pl.when(k != 0)
            def _():
                rad_copy(k).wait_recv()

        for u in range(GROUP):
            p = (me + n - t * GROUP - u) % n
            for s in range(slots):
                l = p * slots + s
                form = form_ref[block_ref[0, l]]
                got = lax.dot_general(
                    fetched_ref[l], form, (((1,), (1,)), ((), ())), preferred_element_type=F32
                )
                fwd_ref[l] = got * live_of(p, s)
        for u in range(GROUP):
            fwd_copy(t * GROUP + u).start()
        return c

    lax.fori_loop(0, n // GROUP, forward, 0)

    def wait_bwd(k, c):
        bwd_copy(k).wait_recv()
        return c

    lax.fori_loop(1, n, wait_bwd, 0)
    most = pl.ds(0, (n - 1) * slots)
    for buf, which in ((bwd_ref, 1), (served_ref, 2)):
        pltpu.make_async_copy(buf.at[most], buf.at[most], send_sems.at[which]).wait()
    rows = asked_vmem.at[pl.ds(0, n - 1)]
    pltpu.make_async_copy(rows, rows, send_sems.at[0]).wait()
    keep_own.wait()
    keep_asked.wait()
    pltpu.make_async_copy(fwd_ref, fwd_hbm, out_sem.at[2]).wait()


def combine(
    n,
    inner,
    target_hbm,
    asked_hbm,
    fwd_hbm,
    arrived_hbm,
    em_ref,
    refl_ref,
    area_ref,
    out_hbm,
    target_ref,
    asked_ref,
    fwd_ref,
    arrived_ref,
    gath,
    ret,
    out_ref,
    in_sem,
    out_sem,
):
    me = lax.axis_index("gx") * inner + lax.axis_index("gy")
    clusters = em_ref.shape[0]
    links = fwd_ref.shape[0]
    slots = links // n
    width = asked_ref.shape[2]
    base = me * slots % width
    parts = out_sem.shape[0]
    step = clusters // parts
    loads = [
        pltpu.make_async_copy(src, dst, in_sem.at[i])
        for i, (src, dst) in enumerate(
            (
                (fwd_hbm, fwd_ref),
                (arrived_hbm, arrived_ref),
                (target_hbm, target_ref),
                (asked_hbm, asked_ref),
            )
        )
    ]
    for load in loads:
        load.start()

    def clear(c, carry):
        gath[c] = jnp.zeros(gath.shape[1:], F32)
        ret[c] = jnp.zeros(ret.shape[1:], F32)
        return carry

    lax.fori_loop(0, clusters, clear, 0, unroll=8)
    for load in loads:
        load.wait()

    def scatter(p, carry):
        for s in range(slots):
            l = p * slots + s
            t = target_ref[0, l]
            c = asked_ref[p, 0, base + s]
            gath[t] += fwd_ref[l]
            ret[c] += arrived_ref[l].astype(F32)
        return carry

    lax.fori_loop(0, n, scatter, 0, unroll=2)

    def finish(c, carry):
        area = area_ref[pl.ds(c, 1), :]
        out_ref[c] = em_ref[c] + refl_ref[c] * (gath[c] + ret[c] / area)
        return carry

    stores = []
    for i in range(parts):
        lax.fori_loop(i * step, (i + 1) * step, finish, 0, unroll=8)
        rows = pl.ds(i * step, step)
        stores.append(pltpu.make_async_copy(out_ref.at[rows], out_hbm.at[rows], out_sem.at[i]))
        stores[-1].start()
    for store in stores:
        store.wait()


def solution(mesh):
    outer, inner = mesh.shape["gx"], mesh.shape["gy"]
    n = outer * inner

    def shards(
        radiance,
        emission,
        reflectance,
        patch_area,
        form_factor,
        source_index,
        target_index,
        block_index,
        valid_count,
    ):
        clusters, bands, patches = radiance.shape
        links = source_index.shape[1]
        slots = links // n
        tile = (bands, patches)
        vm = pl.BlockSpec(memory_space=pltpu.VMEM)
        hbm = pl.BlockSpec(memory_space=pl.ANY)
        width = min(links, LANES)
        parts = 4
        fwd, arrived, asked = pl.pallas_call(
            functools.partial(exchange, n, inner),
            out_shape=(
                jax.ShapeDtypeStruct((links,) + tile, F32),
                jax.ShapeDtypeStruct((links,) + tile, BF16),
                jax.ShapeDtypeStruct((n, 1, width), jnp.int32),
            ),
            in_specs=[hbm] * 7,
            out_specs=(hbm, hbm, hbm),
            scratch_shapes=[
                pltpu.SMEM(block_index.shape, jnp.int32),
                pltpu.SMEM(target_index.shape, jnp.int32),
                pltpu.SMEM(valid_count.shape, jnp.int32),
                pltpu.VMEM(source_index.shape, jnp.int32),
                pltpu.VMEM(radiance.shape, BF16),
                pltpu.VMEM(patch_area.shape, F32),
                pltpu.VMEM(form_factor.shape, BF16),
                pltpu.VMEM((clusters,) + tile, BF16),
                pltpu.VMEM((links,) + tile, BF16),
                pltpu.VMEM((links,) + tile, BF16),
                pltpu.VMEM((links,) + tile, BF16),
                pltpu.VMEM((links,) + tile, F32),
                pltpu.VMEM((n, 1, width), jnp.int32),
                pltpu.SMEM((n, 1, width), jnp.int32),
                pltpu.SemaphoreType.DMA((parts,)),
                pltpu.SemaphoreType.DMA((6,)),
                pltpu.SemaphoreType.DMA((3,)),
                pltpu.SemaphoreType.DMA((3,)),
                pltpu.SemaphoreType.DMA((n,)),
                pltpu.SemaphoreType.DMA((n,)),
                pltpu.SemaphoreType.DMA((n,)),
            ],
            compiler_params=pltpu.CompilerParams(
                collective_id=0, has_side_effects=True, vmem_limit_bytes=EXCHANGE_MIB * 1024 * 1024
            ),
            name="exchange",
        )(
            block_index,
            target_index,
            valid_count,
            source_index,
            radiance,
            patch_area,
            form_factor,
        )
        return pl.pallas_call(
            functools.partial(combine, n, inner),
            out_shape=jax.ShapeDtypeStruct((clusters,) + tile, F32),
            in_specs=[hbm, hbm, hbm, hbm, vm, vm, vm],
            out_specs=hbm,
            scratch_shapes=[
                pltpu.SMEM(target_index.shape, jnp.int32),
                pltpu.SMEM((n, 1, width), jnp.int32),
                pltpu.VMEM((links,) + tile, F32),
                pltpu.VMEM((links,) + tile, BF16),
                pltpu.VMEM((clusters,) + tile, F32),
                pltpu.VMEM((clusters,) + tile, F32),
                pltpu.VMEM((clusters,) + tile, F32),
                pltpu.SemaphoreType.DMA((4,)),
                pltpu.SemaphoreType.DMA((4,)),
            ],
            compiler_params=pltpu.CompilerParams(vmem_limit_bytes=COMBINE_MIB * 1024 * 1024),
            name="combine",
        )(target_index, asked, fwd, arrived, emission, reflectance, patch_area)

    spec3 = P(("gx", "gy"), None, None)
    spec2 = P(("gx", "gy"), None)
    return jax.shard_map(
        shards,
        mesh=mesh,
        in_specs=(spec3, spec3, spec3, spec2, spec3, spec2, spec2, spec2, spec2),
        out_specs=spec3,
        check_vma=False,
    )
```

```python
import functools

import jax
import jax.numpy as jnp
from jax import lax
from jax.experimental import pallas as pl
from jax.experimental.pallas import tpu as pltpu
from jax.sharding import PartitionSpec as P

MESH = pl.DeviceIdType.MESH
GROUP = 4
LANES = 128
EXCHANGE_MIB = 60
COMBINE_MIB = 60
F32 = jnp.float32
BF16 = jnp.bfloat16


def exchange(
    n,
    inner,
    block_hbm,
    target_hbm,
    count_hbm,
    source_hbm,
    rad_hbm,
    area_hbm,
    form_hbm,
    fwd_hbm,
    arrived_hbm,
    asked_hbm,
    block_ref,
    target_ref,
    count_ref,
    source_ref,
    rad_ref,
    area_ref,
    form_ref,
    weighted_ref,
    bwd_ref,
    served_ref,
    fetched_ref,
    fwd_ref,
    asked_vmem,
    asked_ref,
    form_sem,
    in_sem,
    out_sem,
    send_sems,
    idx_sem,
    bwd_sem,
    rad_sem,
):
    me = lax.axis_index("gx") * inner + lax.axis_index("gy")
    links = block_ref.shape[1]
    slots = links // n
    clusters = rad_ref.shape[0]
    parts = form_sem.shape[0]
    step = links // parts

    def coords(p):
        return (p // inner, p % inner)

    loads = [
        pltpu.make_async_copy(src, dst, in_sem.at[i])
        for i, (src, dst) in enumerate(
            (
                (rad_hbm, rad_ref),
                (area_hbm, area_ref),
                (block_hbm, block_ref),
                (target_hbm, target_ref),
                (count_hbm, count_ref),
                (source_hbm, source_ref),
            )
        )
    ]
    forms = [
        pltpu.make_async_copy(
            form_hbm.at[pl.ds(i * step, step)], form_ref.at[pl.ds(i * step, step)], form_sem.at[i]
        )
        for i in range(parts)
    ]
    for load in loads + forms:
        load.start()

    barrier = pltpu.get_barrier_semaphore()

    def greet(k, c):
        pl.semaphore_signal(
            barrier, inc=1, device_id=coords((me + k) % n), device_id_type=MESH
        )
        return c

    lax.fori_loop(1, n, greet, 0)

    for load in loads:
        load.wait()

    def weigh(c, carry):
        area = area_ref[pl.ds(c, 1), :]
        weighted_ref[c] = (area * rad_ref[c].astype(F32)).astype(BF16)
        return carry

    lax.fori_loop(0, clusters, weigh, 0, unroll=8)

    width = asked_vmem.shape[2]

    def lane_base(p):
        if links == width:
            return 0
        return pl.multiple_of(p * slots // width * width, width)

    def idx_copy(k):
        p = (me + k) % n
        return pltpu.make_async_remote_copy(
            src_ref=source_ref.at[:, pl.ds(lane_base(p), width)],
            dst_ref=asked_vmem.at[me],
            send_sem=send_sems.at[0],
            recv_sem=idx_sem.at[k],
            device_id=coords(p),
            device_id_type=MESH,
        )

    def bwd_copy(k):
        p = (me + k) % n
        return pltpu.make_async_remote_copy(
            src_ref=bwd_ref.at[pl.ds(p * slots, slots)],
            dst_ref=arrived_hbm.at[pl.ds(me * slots, slots)],
            send_sem=send_sems.at[1],
            recv_sem=bwd_sem.at[k],
            device_id=coords(p),
            device_id_type=MESH,
        )

    def rad_copy(k):
        p = (me + k) % n
        return pltpu.make_async_remote_copy(
            src_ref=served_ref.at[pl.ds(p * slots, slots)],
            dst_ref=fetched_ref.at[pl.ds(me * slots, slots)],
            send_sem=send_sems.at[2],
            recv_sem=rad_sem.at[k],
            device_id=coords(p),
            device_id_type=MESH,
        )

    def live_of(p, s):
        return jnp.where(s < count_ref[0, p], 1.0, 0.0).astype(F32)

    for form in forms:
        form.wait()

    def back(t):
        for u in range(GROUP):
            p = (me + 1 + t * GROUP + u) % n
            for s in range(slots):
                l = p * slots + s
                form = form_ref[block_ref[0, l]]
                seen = weighted_ref[target_ref[0, l]]
                got = jnp.dot(seen, form, preferred_element_type=F32)
                bwd_ref[l] = (got * live_of(p, s)).astype(BF16)

    def back_only(t, c):
        back(t)
        return c

    def send_bwd(k, c):
        bwd_copy(k).start()
        return c

    def back_send(t, c):
        back(t)
        for u in range(GROUP):
            k = 1 + t * GROUP + u

            @pl.when(k != n)
            def _():
                bwd_copy(k).start()

        return c

    early = n // GROUP // 2
    lax.fori_loop(0, early, back_only, 0)
    pl.semaphore_wait(barrier, n - 1)

    def send_idx(k, c):
        idx_copy(k).start()
        return c

    lax.fori_loop(1, n, send_idx, 0)
    lax.fori_loop(1, 1 + early * GROUP, send_bwd, 0)
    asked_vmem[me] = source_ref[:, pl.ds(lane_base(me), width)]
    lax.fori_loop(early, n // GROUP, back_send, 0)

    own = pl.ds(me * slots, slots)
    keep_own = pltpu.make_async_copy(bwd_ref.at[own], arrived_hbm.at[own], out_sem.at[0])
    keep_own.start()

    def wait_idx(k, c):
        idx_copy(k).wait_recv()
        return c

    lax.fori_loop(1, n, wait_idx, 0)
    to_smem = pltpu.make_async_copy(asked_vmem, asked_ref, out_sem.at[1])
    to_smem.start()
    to_smem.wait()
    base = me * slots % width

    def serve(k, c):
        p = (me + k) % n
        for s in range(slots):
            served_ref[p * slots + s] = rad_ref[asked_ref[p, 0, base + s]]

        @pl.when(k != n)
        def _():
            rad_copy(k).start()

        return c

    lax.fori_loop(1, n + 1, serve, 0)
    for s in range(slots):
        fetched_ref[me * slots + s] = served_ref[me * slots + s]
    keep_asked = pltpu.make_async_copy(asked_vmem, asked_hbm, out_sem.at[1])
    keep_asked.start()

    def fwd_copy(k):
        mine = pl.ds((me + n - k) % n * slots, slots)
        return pltpu.make_async_copy(fwd_ref.at[mine], fwd_hbm.at[mine], out_sem.at[2])

    def forward(t, c):
        for u in range(GROUP):
            k = t * GROUP + u

            @pl.when(k != 0)
            def _():
                rad_copy(k).wait_recv()

        for u in range(GROUP):
            p = (me + n - t * GROUP - u) % n
            for s in range(slots):
                l = p * slots + s
                form = form_ref[block_ref[0, l]]
                got = lax.dot_general(
                    fetched_ref[l], form, (((1,), (1,)), ((), ())), preferred_element_type=F32
                )
                fwd_ref[l] = got * live_of(p, s)
        for u in range(GROUP):
            fwd_copy(t * GROUP + u).start()
        return c

    lax.fori_loop(0, n // GROUP, forward, 0)

    def wait_bwd(k, c):
        bwd_copy(k).wait_recv()
        return c

    lax.fori_loop(1, n, wait_bwd, 0)
    most = pl.ds(0, (n - 1) * slots)
    for buf, which in ((bwd_ref, 1), (served_ref, 2)):
        pltpu.make_async_copy(buf.at[most], buf.at[most], send_sems.at[which]).wait()
    rows = asked_vmem.at[pl.ds(0, n - 1)]
    pltpu.make_async_copy(rows, rows, send_sems.at[0]).wait()
    keep_own.wait()
    keep_asked.wait()
    pltpu.make_async_copy(fwd_ref, fwd_hbm, out_sem.at[2]).wait()


def combine(
    n,
    inner,
    target_hbm,
    asked_hbm,
    fwd_hbm,
    arrived_hbm,
    em_hbm,
    refl_hbm,
    area_hbm,
    out_hbm,
    em_ref,
    refl_ref,
    area_ref,
    target_ref,
    asked_ref,
    fwd_ref,
    arrived_ref,
    gath,
    ret,
    out_ref,
    in_sem,
    out_sem,
):
    me = lax.axis_index("gx") * inner + lax.axis_index("gy")
    clusters = em_ref.shape[0]
    links = fwd_ref.shape[0]
    slots = links // n
    width = asked_ref.shape[2]
    base = me * slots % width
    parts = out_sem.shape[0]
    step = clusters // parts
    loads = [
        pltpu.make_async_copy(src, dst, in_sem.at[i])
        for i, (src, dst) in enumerate(
            (
                (fwd_hbm, fwd_ref),
                (arrived_hbm, arrived_ref),
                (target_hbm, target_ref),
                (asked_hbm, asked_ref),
                (em_hbm, em_ref),
                (refl_hbm, refl_ref),
                (area_hbm, area_ref),
            )
        )
    ]
    for load in loads:
        load.start()

    def clear(c, carry):
        gath[c] = jnp.zeros(gath.shape[1:], F32)
        ret[c] = jnp.zeros(ret.shape[1:], F32)
        return carry

    lax.fori_loop(0, clusters, clear, 0, unroll=8)
    for load in loads[:4]:
        load.wait()

    def scatter(p, carry):
        for s in range(slots):
            l = p * slots + s
            t = target_ref[0, l]
            c = asked_ref[p, 0, base + s]
            gath[t] += fwd_ref[l]
            ret[c] += arrived_ref[l].astype(F32)
        return carry

    lax.fori_loop(0, n, scatter, 0, unroll=2)

    def finish(c, carry):
        area = area_ref[pl.ds(c, 1), :]
        out_ref[c] = em_ref[c] + refl_ref[c] * (gath[c] + ret[c] / area)
        return carry

    for load in loads[4:]:
        load.wait()
    stores = []
    for i in range(parts):
        lax.fori_loop(i * step, (i + 1) * step, finish, 0, unroll=8)
        rows = pl.ds(i * step, step)
        stores.append(pltpu.make_async_copy(out_ref.at[rows], out_hbm.at[rows], out_sem.at[i]))
        stores[-1].start()
    for store in stores:
        store.wait()


def solution(mesh):
    outer, inner = mesh.shape["gx"], mesh.shape["gy"]
    n = outer * inner

    def shards(
        radiance,
        emission,
        reflectance,
        patch_area,
        form_factor,
        source_index,
        target_index,
        block_index,
        valid_count,
    ):
        clusters, bands, patches = radiance.shape
        links = source_index.shape[1]
        slots = links // n
        tile = (bands, patches)
        hbm = pl.BlockSpec(memory_space=pl.ANY)
        width = min(links, LANES)
        parts = 4
        fwd, arrived, asked = pl.pallas_call(
            functools.partial(exchange, n, inner),
            out_shape=(
                jax.ShapeDtypeStruct((links,) + tile, F32),
                jax.ShapeDtypeStruct((links,) + tile, BF16),
                jax.ShapeDtypeStruct((n, 1, width), jnp.int32),
            ),
            in_specs=[hbm] * 7,
            out_specs=(hbm, hbm, hbm),
            scratch_shapes=[
                pltpu.SMEM(block_index.shape, jnp.int32),
                pltpu.SMEM(target_index.shape, jnp.int32),
                pltpu.SMEM(valid_count.shape, jnp.int32),
                pltpu.VMEM(source_index.shape, jnp.int32),
                pltpu.VMEM(radiance.shape, BF16),
                pltpu.VMEM(patch_area.shape, F32),
                pltpu.VMEM(form_factor.shape, BF16),
                pltpu.VMEM((clusters,) + tile, BF16),
                pltpu.VMEM((links,) + tile, BF16),
                pltpu.VMEM((links,) + tile, BF16),
                pltpu.VMEM((links,) + tile, BF16),
                pltpu.VMEM((links,) + tile, F32),
                pltpu.VMEM((n, 1, width), jnp.int32),
                pltpu.SMEM((n, 1, width), jnp.int32),
                pltpu.SemaphoreType.DMA((parts,)),
                pltpu.SemaphoreType.DMA((6,)),
                pltpu.SemaphoreType.DMA((3,)),
                pltpu.SemaphoreType.DMA((3,)),
                pltpu.SemaphoreType.DMA((n,)),
                pltpu.SemaphoreType.DMA((n,)),
                pltpu.SemaphoreType.DMA((n,)),
            ],
            compiler_params=pltpu.CompilerParams(
                collective_id=0, has_side_effects=True, vmem_limit_bytes=EXCHANGE_MIB * 1024 * 1024
            ),
            name="exchange",
        )(
            block_index,
            target_index,
            valid_count,
            source_index,
            radiance,
            patch_area,
            form_factor,
        )
        return pl.pallas_call(
            functools.partial(combine, n, inner),
            out_shape=jax.ShapeDtypeStruct((clusters,) + tile, F32),
            in_specs=[hbm] * 7,
            out_specs=hbm,
            scratch_shapes=[
                pltpu.VMEM((clusters,) + tile, F32),
                pltpu.VMEM((clusters,) + tile, F32),
                pltpu.VMEM(patch_area.shape, F32),
                pltpu.SMEM(target_index.shape, jnp.int32),
                pltpu.SMEM((n, 1, width), jnp.int32),
                pltpu.VMEM((links,) + tile, F32),
                pltpu.VMEM((links,) + tile, BF16),
                pltpu.VMEM((clusters,) + tile, F32),
                pltpu.VMEM((clusters,) + tile, F32),
                pltpu.VMEM((clusters,) + tile, F32),
                pltpu.SemaphoreType.DMA((7,)),
                pltpu.SemaphoreType.DMA((4,)),
            ],
            compiler_params=pltpu.CompilerParams(vmem_limit_bytes=COMBINE_MIB * 1024 * 1024),
            name="combine",
        )(target_index, asked, fwd, arrived, emission, reflectance, patch_area)

    spec3 = P(("gx", "gy"), None, None)
    spec2 = P(("gx", "gy"), None)
    return jax.shard_map(
        shards,
        mesh=mesh,
        in_specs=(spec3, spec3, spec3, spec2, spec3, spec2, spec2, spec2, spec2),
        out_specs=spec3,
        check_vma=False,
    )
```
